32 devices in a mesh: seq: 8 (over z, y), head: 4 (over x, core).
Axes of the slice: x: 2, y: 2, z: 4, core: 2. Of those that a mesh axis runs over, the one named last changes fastest.
Arguments:
- doc_lengths: int32 [32], P(('seq', 'head')), may hold values from 1 to 2688, 6144 in all
- queries: bfloat16 [6144, 8192], P('seq', 'head'), may hold values from -24 to 24
- key_states: bfloat16 [6144, 1024], P('seq', 'head'), may hold values from -24 to 24
- value_states: bfloat16 [6144, 1024], P('seq', 'head'), may hold values from -6 to 6
Outputs:
- attended: bfloat16 [6144, 8192], P('seq', 'head')
The draws below stay inside these ranges and needn't reach their ends.
Inputs may be any that keep to these rules, and one draw needn't show every extreme that they name: `doc_lengths`: the 32 lengths sum to 6144; the largest is exactly 2688.
All inputs are finite; a program needn't handle non-finite values. No bound on the sum of `doc_lengths` on one device may be relied on, other than what follows from the above.
Results may differ from the reference program's by a relative error of at most 0.0028.
Values may be sent and summed in bfloat16 or wider, within the bound.
A program may use at most 64 MiB of HBM per device.

```python
import math
import jax
import jax.numpy as jnp
import numpy as np
from jax import lax

HD = 128
QH = 64
KVH = 8
TILE = 128
GROUP = 8
TOKENS = 6144
DOCS = 32
LONGEST = 2688


def draw_queries(key, part):
    drawn = jnp.clip(jax.random.normal(jax.random.fold_in(key, 1), (TOKENS, QH * HD)), -6.0, 6.0)
    return drawn.astype(jnp.bfloat16)


def draw_key_states(key, part):
    drawn = jnp.clip(jax.random.normal(jax.random.fold_in(key, 2), (TOKENS, KVH * HD)), -6.0, 6.0)
    return drawn.astype(jnp.bfloat16)


def shard_levels(rng, shape, cuts, smallest, top_value):
    def one(dim, shards_of):
        steps = jax.random.uniform(jax.random.fold_in(jax.random.fold_in(rng, 6), dim), (shards_of,), jnp.float32, smallest / len(cuts), top_value / len(cuts))
        return jnp.repeat(jnp.exp(steps), shape[dim] // shards_of).reshape((-1,) + (1,) * (len(shape) - dim - 1))

    gain = one(*cuts[0])
    for cut in cuts[1:]:
        gain = gain * one(*cut)
    return gain


def length_profile(number_of, total, bound, skew):
    weights = [(1 << 20) // math.isqrt(grade ** skew) + 1 for grade in range(2, number_of + 1)]
    rest, counts = total - bound - (number_of - 1), [1] * (number_of - 1)
    while rest > 0:
        candidates = [i for i in range(number_of - 1) if counts[i] < bound]
        whole, remaining = sum([weights[i] for i in candidates]), rest
        for i in candidates:
            extra = min(bound - counts[i], max(1, remaining * weights[i] // whole), rest)
            counts[i] = counts[i] + extra
            rest = rest - extra
    return np.array([bound] + counts)


def ragged(rng, number_of, total, most, skew):
    if number_of == 2:
        one = jax.random.randint(rng, (), max(1, total - most), min(most, total - 1) + 1)
        return jnp.stack([one, total - one])
    tallies = jnp.asarray(length_profile(number_of, total, most, skew), jnp.int32)
    pairs = (number_of - 1) // 2
    giver, taker = tallies[1:1 + 2 * pairs:2], tallies[2:2 + 2 * pairs:2]
    slack = jnp.minimum(giver - 1, most - taker)
    shifted = jax.random.randint(jax.random.fold_in(rng, 1), (pairs,), 0, 1 << 20) % (slack + 1)
    tallies = tallies.at[1:1 + 2 * pairs:2].set(giver - shifted).at[2:2 + 2 * pairs:2].set(taker + shifted)
    return tallies[jax.random.permutation(jax.random.fold_in(rng, 2), number_of)]


def centred(stream_key, shape, deviation, reach, pieces=(), kind=jnp.bfloat16):
    level = shard_levels(stream_key, shape, pieces, -0.22, 0.18) if pieces else 1.0
    values = jax.random.normal(stream_key, shape, jnp.float32) * deviation * level
    return jnp.minimum(jnp.maximum(values, -reach), reach).astype(kind)


def setup_inputs(seed: int = 0) -> dict:
    splits = jax.random.split(jax.random.key(seed), 5)
    return {
        "doc_lengths": ragged(splits[0], DOCS, TOKENS, LONGEST, 2).astype(jnp.int32),
        "queries": draw_queries(jax.random.fold_in(splits[4], 71), 0),
        "key_states": draw_key_states(jax.random.fold_in(splits[4], 71), 0),
        "value_states": centred(splits[3], (TOKENS, KVH * HD), 1.0, 6.0, ((0, 8), (1, 4))),
    }


far_below = -1e+30

def document_start(positions, doc_ends, doc_lengths):
    finished = doc_ends[None, :] <= positions[:, None]
    return lax.optimization_barrier(jnp.sum(jnp.where(finished, doc_lengths[None, :], 0), axis=1)).astype(jnp.int32)

def reference(doc_lengths, queries, key_states, value_states):
    doc_ends = jnp.cumsum(doc_lengths).astype(jnp.int32)
    key_span = LONGEST + TILE
    front_zeros = jnp.zeros((LONGEST, KVH * HD), key_states.dtype)
    padded_keys = jnp.concatenate([front_zeros, key_states], axis=0)
    padded_values = jnp.concatenate([front_zeros, value_states], axis=0)
    score_scale = 1.0 / math.sqrt(HD)

    def one_tile(tile_index):
        first_row = (tile_index * TILE).astype(jnp.int32)
        query_tile = lax.dynamic_slice_in_dim(queries, first_row, TILE, 0).reshape(TILE, KVH, GROUP, HD).astype(jnp.float32)
        key_window = lax.dynamic_slice_in_dim(padded_keys, first_row, key_span, 0).reshape(key_span, KVH, HD).astype(jnp.float32)
        value_window = lax.dynamic_slice_in_dim(padded_values, first_row, key_span, 0).reshape(key_span, KVH, HD).astype(jnp.float32)
        query_pos = first_row + jnp.arange(TILE, dtype=jnp.int32)
        key_pos = first_row - LONGEST + jnp.arange(key_span, dtype=jnp.int32)
        starts = document_start(query_pos, doc_ends, doc_lengths)
        visible = (key_pos[None, :] >= starts[:, None]) & (key_pos[None, :] <= query_pos[:, None])
        scores = jnp.einsum('qhgd,khd->hgqk', query_tile, key_window) * score_scale
        scores = jnp.where(visible, scores, far_below)
        row_max = lax.optimization_barrier(jnp.max(scores, axis=-1, keepdims=True))
        weights = jnp.where(visible, jnp.exp(scores - row_max), 0.0)
        weight_sum = lax.optimization_barrier(jnp.sum(weights, axis=-1, keepdims=True))
        rounded = lax.optimization_barrier(weights.astype(jnp.bfloat16))
        mixed_out = jnp.einsum('hgqk,khd->hgqd', rounded.astype(jnp.float32), value_window) / weight_sum
        return mixed_out.transpose(2, 0, 1, 3).reshape(TILE, QH * HD).astype(jnp.bfloat16)
    all_tiles = lax.map(one_tile, jnp.arange(TOKENS // TILE, dtype=jnp.int32))
    return all_tiles.reshape(TOKENS, QH * HD)
```

```python
import functools
import math

import jax
import jax.numpy as jnp
from jax import lax
from jax.experimental import pallas as pl
from jax.experimental.pallas import tpu as pltpu
from jax.sharding import PartitionSpec as P

HD = 128
TILE = 128
LONGEST = 2688
STEP = 512
CHUNK = 256
AHEAD = 2
DIGIT = 32
NO_KEY = HD - 1
BIG = float(2**20)
MESH = pl.DeviceIdType.MESH

VIA_EVEN = (0, 1)
VIA_ODD = (0,)


def attend(
    n_seq,
    n_head,
    kv_heads,
    group,
    lens_ref,
    q_ref,
    k_ref,
    v_ref,
    out_ref,
    lens,
    qv,
    kv,
    qt,
    kf,
    qf,
    digit_a,
    digit_b,
    acc,
    m_ref,
    l_ref,
    out_v,
    lens_send,
    lens_recv,
    in_sems,
    q_sems,
    send_sems,
    recv_sems,
    out_sems,
):
    rows = k_ref.shape[0]
    pieces = rows // TILE
    back = pl.cdiv(LONGEST, rows)
    kept = (LONGEST - (back - 1) * rows) // TILE
    kv_width = kv_heads * HD
    width = group * TILE
    n_chunks = width // CHUNK
    own = back * rows
    first_key = own - LONGEST
    per = lens_ref.shape[0]

    seq = lax.axis_index("seq")
    head = lax.axis_index("head")
    count = n_seq * n_head
    me = seq * n_head + head
    odd = seq % 2
    is_even = odd == 0
    is_odd = odd == 1

    def device(flat):
        return (flat // n_head, flat % n_head)

    own_rows = pl.ds(own, rows)
    load_k = pltpu.make_async_copy(k_ref, kv.at[own_rows, pl.ds(0, kv_width)], in_sems.at[0])
    load_v = pltpu.make_async_copy(
        v_ref, kv.at[own_rows, pl.ds(kv_width, kv_width)], in_sems.at[1]
    )
    load_lens = pltpu.make_async_copy(lens_ref, lens.at[pl.ds(me * per, per)], in_sems.at[2])
    load_k.start()
    load_v.start()
    load_lens.start()
    load_q = [
        pltpu.make_async_copy(
            q_ref.at[pl.ds(t * TILE, TILE)], qv.at[pl.ds(t * TILE, TILE)], q_sems.at[t]
        )
        for t in range(pieces)
    ]
    for copy in load_q:
        copy.start()

    barrier = pltpu.get_barrier_semaphore()

    def greet(i, carry):
        pl.semaphore_signal(
            barrier, inc=1, device_id=device((me + i) % count), device_id_type=MESH
        )
        return carry

    lax.fori_loop(1, count, greet, 0)

    for rel in range(1, back + 1):
        @pl.when(seq < rel)
        def _():
            begin = own - rel * rows
            skip = 0 if rel < back else (pieces - kept) * TILE
            kv[begin + skip : begin + rows, :] = jnp.zeros((rows - skip, 2 * kv_width), kv.dtype)

    load_k.wait()
    load_v.wait()
    load_lens.wait()
    pl.semaphore_wait(barrier, count - 1)

    def lens_copy(slot, i):
        return pltpu.make_async_remote_copy(
            src_ref=lens.at[pl.ds(slot * per, per)],
            dst_ref=lens.at[pl.ds(slot * per, per)],
            send_sem=lens_send.at[i],
            recv_sem=lens_recv.at[slot],
            device_id=device((me + i) % count),
            device_id_type=MESH,
        )

    def send_lens(i, carry):
        lens_copy(me, i).start()
        return carry

    lax.fori_loop(1, count, send_lens, 0)

    def place(rel, j):
        return kv.at[pl.ds(own - rel * rows + j * TILE, TILE), :]

    def hop(kind, rel_here, rel_there, j, to):
        return pltpu.make_async_remote_copy(
            src_ref=place(rel_here, j),
            dst_ref=place(rel_there, j),
            send_sem=send_sems.at[kind, j],
            recv_sem=recv_sems.at[rel_there, j],
            device_id=(to, head),
            device_id_type=MESH,
        )

    hi = range(pieces - kept, pieces)
    every = range(pieces)
    sends = [
        (0, 0, 2, every, seq + 2, seq + 2 < n_seq),
        (1, 0, 1, every, seq + 1, is_even),
        (2, 2, 3, [j for j in every if j not in VIA_ODD], seq + 1, is_even & (seq >= 2)),
        (3, 2, 1, every, seq - 1, is_odd & (seq >= 2)),
        (4, 2, 4, hi, seq + 2, is_even & (seq >= 2) & (seq + 2 < n_seq)),
        (
            5,
            2,
            4,
            [j for j in every if j in hi or j not in VIA_EVEN],
            seq + 2,
            is_odd & (seq >= 2) & (seq + 2 < n_seq),
        ),
        (6, 1, 3, VIA_EVEN, seq + 2, is_even & (seq >= 2) & (seq + 2 < n_seq)),
        (7, 1, 3, VIA_ODD, seq + 2, is_odd & (seq + 2 < n_seq)),
        (
            8,
            4,
            3,
            [j for j in every if j not in VIA_EVEN],
            seq - 1,
            is_odd & (seq >= 4),
        ),
    ]

    def start_sends(rel, j):
        for kind, here, there, chunks, to, condition in sends:
            if here == rel and j in chunks:
                @pl.when(condition)
                def _():
                    hop(kind, here, there, j, to).start()

    def arrive(rel, j):
        if rel == 4 and j not in hi:
            if j in VIA_EVEN:
                return
            condition = is_odd & (seq >= rel)
        else:
            condition = seq >= rel

        @pl.when(condition)
        def _():
            hop(0, rel, rel, j, (seq + 1) % n_seq).wait_recv()

        start_sends(rel, j)

    for j in every:
        start_sends(0, j)

    for t in range(pieces):
        load_q[t].wait()

    def turn(t, carry):
        for c in range(kv_heads):
            for g in range(group):
                tile = qv[pl.ds(pl.multiple_of(t * TILE, TILE), TILE), pl.ds((c * group + g) * HD, HD)]
                qt[c, :, pl.ds(pl.multiple_of(t * width, TILE) + g * TILE, TILE)] = tile.T
        return carry

    lax.fori_loop(0, pieces, turn, 0)

    def wait_lens(i, carry):
        lens_copy((me + i) % count, i).wait_recv()
        return carry

    lax.fori_loop(1, count, wait_lens, 0)

    n_groups = digit_a.shape[0]
    position = (
        (seq - back) * rows
        + lax.broadcasted_iota(jnp.int32, (n_groups, TILE), 0) * TILE
        + lax.broadcasted_iota(jnp.int32, (n_groups, TILE), 1)
    )

    def count_ends(d, carry):
        end, ids = carry
        end = end + lens[d]
        return end, ids + jnp.where(position >= end, 1, 0)

    _, ids = lax.fori_loop(
        0,
        count * per,
        count_ends,
        (jnp.zeros((1, TILE), jnp.int32), jnp.zeros((n_groups, TILE), jnp.int32)),
    )
    digit_a[...] = jnp.where(position < 0, NO_KEY, DIGIT + ids // DIGIT)
    digit_b[...] = jnp.where(position < 0, NO_KEY, ids % DIGIT)

    feature = lax.broadcasted_iota(jnp.int32, (HD, TILE), 0)

    def match(g):
        return (feature == digit_a[pl.ds(g, 1), :]) | (feature == digit_b[pl.ds(g, 1), :])

    def key_features(g, carry):
        one_hot = jnp.where(match(g), 1.0, 0.0).astype(jnp.bfloat16)
        kf[pl.ds(pl.multiple_of(g * TILE, TILE), TILE), :] = one_hot.T
        return carry

    lax.fori_loop(first_key // TILE, (own + rows) // TILE, key_features, 0)

    def query_features(t, carry):
        away = jnp.where(match(own // TILE + t), 0.0, -BIG).astype(jnp.bfloat16)
        for i in range(CHUNK // TILE):
            qf[:, pl.ds(pl.multiple_of(t * CHUNK, TILE) + i * TILE, TILE)] = away
        return carry

    lax.fori_loop(0, pieces, query_features, 0)

    scale = math.log2(math.e) / math.sqrt(HD)

    def block(t, begin, n_keys, first):
        flags = kf[pl.ds(begin, n_keys), :]
        marks = qf[:, pl.ds(pl.multiple_of(t * CHUNK, TILE), CHUNK)]
        keys, values = [], []
        for c in range(kv_heads):
            keys.append(
                jnp.concatenate([kv[pl.ds(begin, n_keys), pl.ds(c * HD, HD)], flags], axis=1)
            )
            values.append(kv[pl.ds(begin, n_keys), pl.ds(kv_width + c * HD, HD)].T)
        if first:
            tail = 2 * TILE
            key_row = begin + n_keys - tail + lax.broadcasted_iota(jnp.int32, (tail, CHUNK), 0)
            query_row = own + t * TILE + lax.broadcasted_iota(jnp.int32, (tail, CHUNK), 1) % TILE
            later = key_row > query_row
        units = [(c, i) for c in range(kv_heads) for i in range(n_chunks)]

        def lanes(i):
            return pl.ds(pl.multiple_of(t * width, TILE) + i * CHUNK, CHUNK)

        def score(unit):
            c, i = unit
            queries = jnp.concatenate([qt[c, :, lanes(i)], marks], axis=0)
            return jnp.dot(keys[c], queries, preferred_element_type=jnp.float32)

        ready = [score(unit) for unit in units[:AHEAD]]
        for at, (c, i) in enumerate(units):
            if at + AHEAD < len(units):
                ready.append(score(units[at + AHEAD]))
            scores = ready.pop(0)
            if first:
                end = jnp.where(later, -BIG, scores[n_keys - tail :])
                scores = jnp.concatenate([scores[: n_keys - tail], end], axis=0) if n_keys > tail else end
            top = jnp.max(scores, axis=0, keepdims=True)
            if first:
                new_max = top
            else:
                old_max = m_ref[c, :, lanes(i)]
                new_max = jnp.maximum(old_max, top)
            weights = jnp.exp2((scores - new_max) * scale)
            part_sum = jnp.sum(weights.reshape(n_keys // 8, 8, CHUNK), axis=0)
            update = jnp.dot(
                values[c], weights.astype(jnp.bfloat16), preferred_element_type=jnp.float32
            )
            if first:
                l_ref[c, :, lanes(i)] = part_sum
                acc[c, :, lanes(i)] = update
            else:
                shrink = jnp.exp2((old_max - new_max) * scale)
                l_ref[c, :, lanes(i)] = l_ref[c, :, lanes(i)] * shrink + part_sum
                acc[c, :, lanes(i)] = acc[c, :, lanes(i)] * shrink + update
            m_ref[c, :, lanes(i)] = new_max

    events = [[(2, 0)], [(2, 1)], [(2, 2), (2, 3)]]
    for pair in range(pieces // 2):
        def own_tile(t, carry):
            block(t, own, (pair + 1) * 2 * TILE, True)
            return carry

        lax.fori_loop(2 * pair, 2 * pair + 2, own_tile, 0)
        for rel, j in events[min(pair, 2)]:
            arrive(rel, j)

    mid_events = {
        2: [(1, 0), (1, 1)],
        4: [(2, 4)],
        5: [(1, 2), (2, 5)],
        8: [(4, 2), (1, 3)],
        10: [(1, 4), (4, 3)],
        11: [(1, 5)],
        13: [(4, 4)],
        15: [(4, 5)],
        17: [(3, 2), (3, 3), (3, 4), (3, 5)],
    }
    mid_begin = own - 2 * rows

    def mid(it, carry):
        block(it % pieces, pl.multiple_of(mid_begin + (it // pieces) * STEP, TILE), STEP, False)
        for at, arrivals in mid_events.items():
            @pl.when(it == at)
            def _():
                for rel, j in arrivals:
                    arrive(rel, j)
        return carry

    lax.fori_loop(0, 3 * pieces, mid, 0)

    def far(it, carry):
        block(
            it % pieces, pl.multiple_of(mid_begin - STEP - (it // pieces) * STEP, TILE), STEP, False
        )
        @pl.when(it == 0)
        def _():
            for rel, j in [(3, 0), (3, 1)]:
                arrive(rel, j)
        return carry

    lax.fori_loop(0, pieces + 4, far, 0)

    block(0, first_key, TILE, False)
    block(4, first_key + 4 * TILE, TILE, False)

    def finish(t, carry):
        for c in range(kv_heads):
            for g in range(group):
                lanes = pl.ds(pl.multiple_of(t * width, TILE) + g * TILE, TILE)
                total = jnp.sum(l_ref[c, :, lanes], axis=0, keepdims=True)
                result = acc[c, :, lanes] * (1.0 / total)
                out_v[pl.ds(pl.multiple_of(t * TILE, TILE), TILE), pl.ds((c * group + g) * HD, HD)] = (
                    result.T.astype(jnp.bfloat16)
                )
        tile_rows = pl.ds(pl.multiple_of(t * TILE, TILE), TILE)
        pltpu.make_async_copy(out_v.at[tile_rows], out_ref.at[tile_rows], out_sems.at[t]).start()
        return carry

    lax.fori_loop(0, pieces, finish, 0)

    for kind, here, there, chunks, to, condition in sends:
        @pl.when(condition)
        def _():
            for j in chunks:
                hop(kind, here, there, j, to).wait_send()

    def drain_lens(i, carry):
        lens_copy(me, i).wait_send()
        return carry

    lax.fori_loop(1, count, drain_lens, 0)

    def drain_out(t, carry):
        tile_rows = pl.ds(pl.multiple_of(t * TILE, TILE), TILE)
        pltpu.make_async_copy(out_v.at[tile_rows], out_ref.at[tile_rows], out_sems.at[t]).wait()
        return carry

    lax.fori_loop(0, pieces, drain_out, 0)


def body(n_seq, n_head, doc_lengths, queries, key_states, value_states):
    rows, q_width = queries.shape
    pieces = rows // TILE
    kv_heads = key_states.shape[1] // HD
    group = q_width // (kv_heads * HD)
    back = pl.cdiv(LONGEST, rows)
    window = (back + 1) * rows
    per = doc_lengths.shape[0]
    count = n_seq * n_head
    columns = pieces * group * TILE
    lens = jnp.broadcast_to(doc_lengths[:, None, None], (per, 1, TILE))
    kernel = functools.partial(attend, n_seq, n_head, kv_heads, group)
    return pl.pallas_call(
        kernel,
        out_shape=jax.ShapeDtypeStruct(queries.shape, jnp.bfloat16),
        in_specs=[pl.BlockSpec(memory_space=pl.ANY)] * 4,
        out_specs=pl.BlockSpec(memory_space=pl.ANY),
        scratch_shapes=[
            pltpu.VMEM((count * per, 1, TILE), jnp.int32),
            pltpu.VMEM((rows, q_width), jnp.bfloat16),
            pltpu.VMEM((window, 2 * kv_heads * HD), jnp.bfloat16),
            pltpu.VMEM((kv_heads, HD, columns), jnp.bfloat16),
            pltpu.VMEM((window, HD), jnp.bfloat16),
            pltpu.VMEM((HD, pieces * CHUNK), jnp.bfloat16),
            pltpu.VMEM((window // TILE, TILE), jnp.int32),
            pltpu.VMEM((window // TILE, TILE), jnp.int32),
            pltpu.VMEM((kv_heads, HD, columns), jnp.float32),
            pltpu.VMEM((kv_heads, 1, columns), jnp.float32),
            pltpu.VMEM((kv_heads, 8, columns), jnp.float32),
            pltpu.VMEM((rows, q_width), jnp.bfloat16),
            pltpu.SemaphoreType.DMA((count,)),
            pltpu.SemaphoreType.DMA((count,)),
            pltpu.SemaphoreType.DMA((3,)),
            pltpu.SemaphoreType.DMA((pieces,)),
            pltpu.SemaphoreType.DMA((9, pieces)),
            pltpu.SemaphoreType.DMA((back + 1, pieces)),
            pltpu.SemaphoreType.DMA((pieces,)),
        ],
        compiler_params=pltpu.CompilerParams(
            collective_id=0, has_side_effects=True, vmem_limit_bytes=56 * 1024 * 1024
        ),
    )(lens, queries, key_states, value_states)


def solution(mesh):
    return jax.shard_map(
        functools.partial(body, mesh.shape["seq"], mesh.shape["head"]),
        mesh=mesh,
        in_specs=(P(("seq", "head")), P("seq", "head"), P("seq", "head"), P("seq", "head")),
        out_specs=P("seq", "head"),
        check_vma=False,
    )
```

```python
import functools
import math

import jax
import jax.numpy as jnp
from jax import lax
from jax.experimental import pallas as pl
from jax.experimental.pallas import tpu as pltpu
from jax.sharding import PartitionSpec as P

HD = 128
TILE = 128
LONGEST = 2688
CHUNK = 256
SLOTS = 8
PS = 2
DIGIT = 32
NO_KEY = HD - 1
BIG = float(2**20)
MESH = pl.DeviceIdType.MESH

VIA_EVEN = (0, 1)
VIA_ODD = (0,)


def attend(
    n_seq,
    n_head,
    kv_heads,
    group,
    lens_ref,
    q_ref,
    k_ref,
    v_ref,
    out_ref,
    lens,
    qv,
    kv,
    qt,
    kf,
    qf,
    digit_a,
    digit_b,
    acc,
    m_ref,
    s_buf,
    p_buf,
    m_now,
    shrink,
    lens_send,
    lens_recv,
    in_sems,
    q_sems,
    send_sems,
    recv_sems,
):
    rows = k_ref.shape[0]
    pieces = rows // TILE
    back = pl.cdiv(LONGEST, rows)
    kept = (LONGEST - (back - 1) * rows) // TILE
    kv_width = kv_heads * HD
    width = group * TILE
    n_chunks = width // CHUNK
    own = back * rows
    first_key = own - LONGEST
    per = lens_ref.shape[0]

    seq = lax.axis_index("seq")
    head = lax.axis_index("head")
    count = n_seq * n_head
    me = seq * n_head + head
    odd = seq % 2
    is_even = odd == 0
    is_odd = odd == 1

    own_rows = pl.ds(own, rows)
    load_k = pltpu.make_async_copy(k_ref, kv.at[own_rows, pl.ds(0, kv_width)], in_sems.at[0])
    load_v = pltpu.make_async_copy(
        v_ref, kv.at[own_rows, pl.ds(kv_width, kv_width)], in_sems.at[1]
    )
    load_k.start()
    load_v.start()
    load_q = [
        pltpu.make_async_copy(
            q_ref.at[pl.ds(t * TILE, TILE)], qv.at[pl.ds(t * TILE, TILE)], q_sems.at[t]
        )
        for t in range(pieces)
    ]
    for copy in load_q:
        copy.start()

    barrier = pltpu.get_barrier_semaphore()
    offsets = [(a, b) for a in range(n_seq) for b in range(n_head) if a or b]

    def peer(offset):
        return ((seq + offset[0]) % n_seq, (head + offset[1]) % n_head)

    for offset in offsets:
        pl.semaphore_signal(barrier, inc=1, device_id=peer(offset), device_id_type=MESH)

    for i in range(per):
        lens[me * per + i] = jnp.full((1, TILE), lens_ref[i], jnp.int32)

    for rel in range(1, back + 1):
        @pl.when(seq < rel)
        def _():
            begin = own - rel * rows
            skip = 0 if rel < back else (pieces - kept) * TILE
            kv[begin + skip : begin + rows, :] = jnp.zeros((rows - skip, 2 * kv_width), kv.dtype)

    load_k.wait()
    load_v.wait()
    pl.semaphore_wait(barrier, count - 1)

    def lens_copy(slot, i):
        return pltpu.make_async_remote_copy(
            src_ref=lens.at[pl.ds(slot * per, per)],
            dst_ref=lens.at[pl.ds(slot * per, per)],
            send_sem=lens_send.at[i],
            recv_sem=lens_recv.at[slot],
            device_id=peer(offsets[i]),
            device_id_type=MESH,
        )

    def place(rel, j):
        return kv.at[pl.ds(own - rel * rows + j * TILE, TILE), :]

    def hop(kind, rel_here, rel_there, j, to):
        return pltpu.make_async_remote_copy(
            src_ref=place(rel_here, j),
            dst_ref=place(rel_there, j),
            send_sem=send_sems.at[kind, j],
            recv_sem=recv_sems.at[rel_there, j],
            device_id=(to, head),
            device_id_type=MESH,
        )

    hi = range(pieces - kept, pieces)
    every = range(pieces)
    sends = [
        (0, 0, 2, every, seq + 2, seq + 2 < n_seq),
        (1, 0, 1, every, seq + 1, is_even),
        (2, 2, 3, [j for j in every if j not in VIA_ODD], seq + 1, is_even & (seq >= 2)),
        (3, 2, 1, every, seq - 1, is_odd & (seq >= 2)),
        (4, 2, 4, hi, seq + 2, is_even & (seq >= 2) & (seq + 2 < n_seq)),
        (
            5,
            2,
            4,
            [j for j in every if j in hi or j not in VIA_EVEN],
            seq + 2,
            is_odd & (seq >= 2) & (seq + 2 < n_seq),
        ),
        (6, 1, 3, VIA_EVEN, seq + 2, is_even & (seq >= 2) & (seq + 2 < n_seq)),
        (7, 1, 3, VIA_ODD, seq + 2, is_odd & (seq + 2 < n_seq)),
        (
            8,
            4,
            3,
            [j for j in every if j not in VIA_EVEN],
            seq - 1,
            is_odd & (seq >= 4),
        ),
    ]

    def start_sends(rel, j):
        for kind, here, there, chunks, to, condition in sends:
            if here == rel and j in chunks:
                @pl.when(condition)
                def _():
                    hop(kind, here, there, j, to).start()

    def arrive(rel, j):
        if rel == 4 and j not in hi:
            if j in VIA_EVEN:
                return
            condition = is_odd & (seq >= rel)
        else:
            condition = seq >= rel

        @pl.when(condition)
        def _():
            hop(0, rel, rel, j, (seq + 1) % n_seq).wait_recv()

        start_sends(rel, j)

    for i in range(count - 1):
        lens_copy(me, i).start()
    for j in every:
        start_sends(0, j)

    for t in range(pieces):
        load_q[t].wait()

    def turn(t, carry):
        for c in range(kv_heads):
            for g in range(group):
                tile = qv[pl.ds(pl.multiple_of(t * TILE, TILE), TILE), pl.ds((c * group + g) * HD, HD)]
                qt[c, :, pl.ds(pl.multiple_of(t * width, TILE) + g * TILE, TILE)] = tile.T
        return carry

    lax.fori_loop(0, pieces, turn, 0)

    for i in range(count - 1):
        there = peer(offsets[i])
        lens_copy(there[0] * n_head + there[1], i).wait_recv()

    n_groups = digit_a.shape[0]
    position = (
        (seq - back) * rows
        + lax.broadcasted_iota(jnp.int32, (n_groups, TILE), 0) * TILE
        + lax.broadcasted_iota(jnp.int32, (n_groups, TILE), 1)
    )

    ends_step = 8

    def count_ends(k, carry):
        end, ids = carry
        for i in range(ends_step):
            end = end + lens[k * ends_step + i]
            ids = ids + jnp.where(position >= end, 1, 0)
        return end, ids

    _, ids = lax.fori_loop(
        0,
        count * per // ends_step,
        count_ends,
        (jnp.zeros((1, TILE), jnp.int32), jnp.zeros((n_groups, TILE), jnp.int32)),
    )
    digit_a[...] = jnp.where(position < 0, NO_KEY, DIGIT + ids // DIGIT)
    digit_b[...] = jnp.where(position < 0, NO_KEY, ids % DIGIT)

    feature = lax.broadcasted_iota(jnp.int32, (HD, TILE), 0)

    def match(g):
        return (feature == digit_a[g : g + 1, :]) | (feature == digit_b[g : g + 1, :])

    def key_features(g):
        one_hot = jnp.where(match(g), 1.0, 0.0).astype(jnp.bfloat16)
        kf[g * TILE : (g + 1) * TILE, :] = one_hot.T

    for t in range(pieces):
        key_features(own // TILE + t)
        away = jnp.where(match(own // TILE + t), 0.0, -BIG).astype(jnp.bfloat16)
        for i in range(CHUNK // TILE):
            qf[:, t * CHUNK + i * TILE : t * CHUNK + (i + 1) * TILE] = away

    scale = math.log2(math.e) / math.sqrt(HD)
    units = [(a, c, i) for a in range(2) for c in range(kv_heads) for i in range(n_chunks)]
    one = len(units) // 2
    slots = s_buf.shape[0]
    ahead = slots - 1

    def lanes(t, i):
        return pl.ds(pl.multiple_of(t * width, TILE) + i * CHUNK, CHUNK)

    def scores(k, u, t, slabs, first):
        a, c, i = units[u]
        t = t + a
        marks = qf[:, pl.ds(pl.multiple_of(t * CHUNK, TILE), CHUNK)]
        keys = jnp.concatenate(
            [
                jnp.concatenate([kv[pl.ds(at, n), pl.ds(c * HD, HD)], kf[pl.ds(at, n), :]], axis=1)
                for at, n in slabs
            ],
            axis=0,
        )
        queries = jnp.concatenate([qt[c, :, lanes(t, i)], marks], axis=0)
        result = jnp.dot(keys, queries, preferred_element_type=jnp.float32)
        n_keys = result.shape[0]
        if first:
            key = lax.broadcasted_iota(jnp.int32, (TILE, CHUNK), 0)
            query = lax.broadcasted_iota(jnp.int32, (TILE, CHUNK), 1) % TILE
            end = jnp.where(key > query, -BIG, result[n_keys - TILE :])
            result = jnp.concatenate([result[: n_keys - TILE], end], axis=0) if n_keys > TILE else end
        s_buf[k % slots, :n_keys, :] = result
        top = jnp.max(result, axis=0, keepdims=True)
        if not first:
            old_max = m_ref[c, :, lanes(t, i)]
            top = jnp.maximum(old_max, top)
            shrink[k % len(units)] = jnp.exp2((old_max - top) * scale)
        m_now[k % len(units)] = top
        m_ref[c, :, lanes(t, i)] = top

    def weigh(k, u, t, n_keys, first):
        a, c, i = units[u]
        t = t + a
        top = m_now[k % len(units)]
        for r in range(0, n_keys, TILE):
            weights = jnp.exp2((s_buf[k % slots, r : r + TILE, :] - top) * scale)
            p_buf[k % PS, r : r + TILE, :] = weights.astype(jnp.bfloat16)

    def add_values(k, u, t, slabs, first):
        a, c, i = units[u]
        t = t + a
        values = jnp.concatenate(
            [kv[pl.ds(at, n), pl.ds(kv_width + c * HD, HD)].T for at, n in slabs], axis=1
        )
        n_keys = values.shape[1]
        values = jnp.concatenate([values, jnp.ones((16, n_keys), values.dtype)], axis=0)
        weights = p_buf[k % PS, :n_keys, :]
        update = jnp.dot(values, weights, preferred_element_type=jnp.float32)[: HD + 8]
        if first:
            acc[c, :, lanes(t, i)] = update
        else:
            acc[c, :, lanes(t, i)] = acc[c, :, lanes(t, i)] * shrink[k % len(units)] + update

    earlier = list(range(first_key // TILE, own // TILE))
    share = pl.cdiv(len(earlier), pieces - 1)
    events = {2: [(2, 0)], pieces - 2: [(2, 1)], pieces - 1: [(2, 2), (2, 3)]}
    items = [(t, u) for t in range(pieces) for u in range(one)]

    def item(k):
        t, u = items[k]
        return u, t, [(own, (t + 1) * TILE)]

    for k in range(ahead):
        scores(k, *item(k), True)
    for k, (t, u) in enumerate(items):
        if k + ahead < len(items):
            scores(k + ahead, *item(k + ahead), True)
        if k:
            add_values(k - 1, *item(k - 1), True)
        weigh(k, u, t, (t + 1) * TILE, True)
        if u == one - 1:
            for g in earlier[t * share : (t + 1) * share]:
                key_features(g)
            for rel, j in events.get(t, []):
                arrive(rel, j)
    add_values(len(items) - 1, *item(len(items) - 1), True)

    n_step = 4 * TILE
    pairs = pieces // 2
    steps = 5 * pairs - 1

    def where(it):
        it = it + it // (4 * pairs - 1)
        stage = it // pairs
        begin = own - 2 * rows + (stage - stage // 3 * 5) * n_step
        return 2 * (it % pairs), [(pl.multiple_of(begin, TILE), n_step)]

    step_events = {
        0: [(1, 0)],
        1: [(1, 1)],
        2: [(2, 4), (2, 5)],
        3: [(1, 2)],
        4: [(1, 3), (4, 2)],
        5: [(1, 4), (1, 5), (4, 3)],
        6: [(4, 4)],
        7: [(4, 5)],
        8: [(3, 0), (3, 1)],
        10: [(3, 2), (3, 3), (3, 4), (3, 5)],
    }

    def hook(it):
        for low in (0, 4, 8):
            @pl.when(it // 4 == low // 4)
            def _():
                for at, arrivals in step_events.items():
                    if low <= at < low + 4:
                        @pl.when(it == at)
                        def _():
                            for rel, j in arrivals:
                                arrive(rel, j)

    n_units = len(units)
    last = n_units - 1
    for u in range(ahead):
        scores(u, u, *where(0), False)
    p_buf[last % PS] = jnp.zeros(p_buf.shape[1:], p_buf.dtype)
    shrink[last] = jnp.ones((1, CHUNK), jnp.float32)

    def step(it, carry):
        hook(it)
        now, then = where(it), where(it + 1 - (it + 1) // steps)
        before = where(it - (it + steps - 1) // steps)
        for u in range(n_units):
            later = u + ahead
            scores(later, later % n_units, *(now if later < n_units else then), False)
            add_values(u - 1, (u - 1) % n_units, *(now if u else before), False)
            weigh(u, u, now[0], n_step, False)
        return carry

    lax.fori_loop(0, steps, step, 0)
    add_values(last, last, *where(steps - 1), False)

    def finish(t):
        for c in range(kv_heads):
            for g in range(group):
                at = slice(t * width + g * TILE, t * width + (g + 1) * TILE)
                result = (acc[c, :HD, at] * (1.0 / acc[c, HD : HD + 1, at])).astype(jnp.bfloat16)
                columns = slice((c * group + g) * HD, (c * group + g + 1) * HD)
                out_ref[t * TILE : (t + 1) * TILE, columns] = result.T

    ends = [(0, first_key), (4, first_key + n_step)]
    items = [(t, u, [(at, TILE)]) for t, at in ends for u in range(one)]
    others = [t for t in range(pieces) if t not in (0, 4)]
    for k, (t, u, slabs) in enumerate(items[:ahead]):
        scores(k, u, t, slabs, False)
    for k, (t, u, slabs) in enumerate(items):
        if k + ahead < len(items):
            scores(k + ahead, *[items[k + ahead][i] for i in (1, 0, 2)], False)
        weigh(k, u, t, TILE, False)
        add_values(k, u, t, slabs, False)
        if k % 2 and k // 2 < len(others):
            finish(others[k // 2])
    finish(0)
    finish(4)

    for kind, here, there, chunks, to, condition in sends:
        @pl.when(condition)
        def _():
            for j in chunks:
                hop(kind, here, there, j, to).wait_send()

    for i in range(count - 1):
        lens_copy(me, i).wait_send()


def body(n_seq, n_head, doc_lengths, queries, key_states, value_states):
    rows, q_width = queries.shape
    pieces = rows // TILE
    kv_heads = key_states.shape[1] // HD
    group = q_width // (kv_heads * HD)
    back = pl.cdiv(LONGEST, rows)
    window = (back + 1) * rows
    per = doc_lengths.shape[0]
    count = n_seq * n_head
    columns = pieces * group * TILE
    units = 2 * kv_heads * group * TILE // CHUNK
    kernel = functools.partial(attend, n_seq, n_head, kv_heads, group)
    return pl.pallas_call(
        kernel,
        out_shape=pltpu.VMEM(queries.shape, jnp.bfloat16),
        in_specs=[pl.BlockSpec(memory_space=pltpu.SMEM)]
        + [pl.BlockSpec(memory_space=pl.ANY)] * 3,
        out_specs=pl.BlockSpec(memory_space=pltpu.VMEM),
        scratch_shapes=[
            pltpu.VMEM((count * per, 1, TILE), jnp.int32),
            pltpu.VMEM((rows, q_width), jnp.bfloat16),
            pltpu.VMEM((window, 2 * kv_heads * HD), jnp.bfloat16),
            pltpu.VMEM((kv_heads, HD, columns), jnp.bfloat16),
            pltpu.VMEM((window, HD), jnp.bfloat16),
            pltpu.VMEM((HD, pieces * CHUNK), jnp.bfloat16),
            pltpu.VMEM((window // TILE, TILE), jnp.int32),
            pltpu.VMEM((window // TILE, TILE), jnp.int32),
            pltpu.VMEM((kv_heads, HD + 8, columns), jnp.float32),
            pltpu.VMEM((kv_heads, 1, columns), jnp.float32),
            pltpu.VMEM((SLOTS, rows, CHUNK), jnp.float32),
            pltpu.VMEM((PS, rows, CHUNK), jnp.bfloat16),
            pltpu.VMEM((units, 1, CHUNK), jnp.float32),
            pltpu.VMEM((units, 1, CHUNK), jnp.float32),
            pltpu.SemaphoreType.DMA((count,)),
            pltpu.SemaphoreType.DMA((count,)),
            pltpu.SemaphoreType.DMA((2,)),
            pltpu.SemaphoreType.DMA((pieces,)),
            pltpu.SemaphoreType.DMA((9, pieces)),
            pltpu.SemaphoreType.DMA((back + 1, pieces)),
        ],
        compiler_params=pltpu.CompilerParams(
            collective_id=0, has_side_effects=True, vmem_limit_bytes=56 * 1024 * 1024
        ),
    )(doc_lengths, queries, key_states, value_states)


def solution(mesh):
    return jax.shard_map(
        functools.partial(body, mesh.shape["seq"], mesh.shape["head"]),
        mesh=mesh,
        in_specs=(P(("seq", "head")), P("seq", "head"), P("seq", "head"), P("seq", "head")),
        out_specs=P("seq", "head"),
        check_vma=False,
    )
```

```python
import functools
import math

import jax
import jax.numpy as jnp
from jax import lax
from jax.experimental import pallas as pl
from jax.experimental.pallas import tpu as pltpu
from jax.sharding import PartitionSpec as P

HD = 128
TILE = 128
LONGEST = 2688
CHUNK = 256
SLOTS = 8
PS = 2
DIGIT = 32
NO_KEY = HD - 1
BIG = float(2**20)
MESH = pl.DeviceIdType.MESH

VIA_EVEN = (0, 1)
VIA_ODD = (0,)


def attend(
    n_seq,
    n_head,
    kv_heads,
    group,
    lens_ref,
    q_ref,
    k_ref,
    v_ref,
    out_ref,
    lens,
    qv,
    kv,
    qt,
    kf,
    qf,
    digit_a,
    digit_b,
    acc,
    m_ref,
    s_buf,
    p_buf,
    m_now,
    shrink,
    lens_sems,
    in_sems,
    q_sems,
    send_sems,
    recv_sems,
):
    rows = k_ref.shape[0]
    pieces = rows // TILE
    back = pl.cdiv(LONGEST, rows)
    kept = (LONGEST - (back - 1) * rows) // TILE
    kv_width = kv_heads * HD
    width = group * TILE
    n_chunks = width // CHUNK
    own = back * rows
    first_key = own - LONGEST
    per = lens_ref.shape[0]

    seq = lax.axis_index("seq")
    head = lax.axis_index("head")
    count = n_seq * n_head
    me = seq * n_head + head
    odd = seq % 2
    is_even = odd == 0
    is_odd = odd == 1

    own_rows = pl.ds(own, rows)
    load_k = pltpu.make_async_copy(k_ref, kv.at[own_rows, pl.ds(0, kv_width)], in_sems.at[0])
    load_v = pltpu.make_async_copy(
        v_ref, kv.at[own_rows, pl.ds(kv_width, kv_width)], in_sems.at[1]
    )
    load_k.start()
    load_v.start()
    load_q = [
        pltpu.make_async_copy(
            q_ref.at[pl.ds(t * TILE, TILE)], qv.at[pl.ds(t * TILE, TILE)], q_sems.at[t]
        )
        for t in range(pieces)
    ]
    for copy in load_q:
        copy.start()

    barrier = pltpu.get_barrier_semaphore()
    offsets = [(a, b) for a in range(n_seq) for b in range(n_head) if a or b]

    def peer(offset):
        return ((seq + offset[0]) % n_seq, (head + offset[1]) % n_head)

    for offset in offsets:
        pl.semaphore_signal(barrier, inc=1, device_id=peer(offset), device_id_type=MESH)

    for i in range(per):
        lens[me * per + i] = jnp.full((1, TILE), lens_ref[i], jnp.int32)

    for rel in range(1, back + 1):
        @pl.when(seq < rel)
        def _():
            begin = own - rel * rows
            skip = 0 if rel < back else (pieces - kept) * TILE
            kv[begin + skip : begin + rows, :] = jnp.zeros((rows - skip, 2 * kv_width), kv.dtype)

    load_k.wait()
    load_v.wait()
    pl.semaphore_wait(barrier, count - 1)

    def lens_copy(slot, i):
        return pltpu.make_async_remote_copy(
            src_ref=lens.at[pl.ds(slot * per, per)],
            dst_ref=lens.at[pl.ds(slot * per, per)],
            send_sem=lens_sems.at[0],
            recv_sem=lens_sems.at[1],
            device_id=peer(offsets[i]),
            device_id_type=MESH,
        )

    def place(rel, j):
        return kv.at[pl.ds(own - rel * rows + j * TILE, TILE), :]

    def hop(kind, rel_here, rel_there, j, to):
        return pltpu.make_async_remote_copy(
            src_ref=place(rel_here, j),
            dst_ref=place(rel_there, j),
            send_sem=send_sems.at[kind],
            recv_sem=recv_sems.at[rel_there, j],
            device_id=(to, head),
            device_id_type=MESH,
        )

    hi = range(pieces - kept, pieces)
    every = range(pieces)
    sends = [
        (0, 0, 2, every, seq + 2, seq + 2 < n_seq),
        (1, 0, 1, every, seq + 1, is_even),
        (2, 2, 3, [j for j in every if j not in VIA_ODD], seq + 1, is_even & (seq >= 2)),
        (3, 2, 1, every, seq - 1, is_odd & (seq >= 2)),
        (4, 2, 4, hi, seq + 2, is_even & (seq >= 2) & (seq + 2 < n_seq)),
        (
            5,
            2,
            4,
            [j for j in every if j in hi or j not in VIA_EVEN],
            seq + 2,
            is_odd & (seq >= 2) & (seq + 2 < n_seq),
        ),
        (6, 1, 3, VIA_EVEN, seq + 2, is_even & (seq >= 2) & (seq + 2 < n_seq)),
        (7, 1, 3, VIA_ODD, seq + 2, is_odd & (seq + 2 < n_seq)),
        (
            8,
            4,
            3,
            [j for j in every if j not in VIA_EVEN],
            seq - 1,
            is_odd & (seq >= 4),
        ),
    ]

    def start_sends(rel, j):
        for kind, here, there, chunks, to, condition in sends:
            if here == rel and j in chunks:
                @pl.when(condition)
                def _():
                    hop(kind, here, there, j, to).start()

    def arrive(rel, j):
        if rel == 4 and j not in hi:
            if j in VIA_EVEN:
                return
            condition = is_odd & (seq >= rel)
        else:
            condition = seq >= rel

        @pl.when(condition)
        def _():
            hop(0, rel, rel, j, (seq + 1) % n_seq).wait_recv()

        start_sends(rel, j)

    for i in range(count - 1):
        lens_copy(me, i).start()
    for j in every:
        start_sends(0, j)

    for t in range(pieces):
        load_q[t].wait()

    def turn(t, carry):
        for c in range(kv_heads):
            for g in range(group):
                tile = qv[pl.ds(pl.multiple_of(t * TILE, TILE), TILE), pl.ds((c * group + g) * HD, HD)]
                qt[c, :, pl.ds(pl.multiple_of(t * width, TILE) + g * TILE, TILE)] = tile.T
        return carry

    lax.fori_loop(0, pieces, turn, 0)

    def all_lens():
        others = lens.at[pl.ds(0, (count - 1) * per)]
        return pltpu.make_async_remote_copy(
            src_ref=others,
            dst_ref=others,
            send_sem=lens_sems.at[0],
            recv_sem=lens_sems.at[1],
            device_id=peer(offsets[0]),
            device_id_type=MESH,
        )

    all_lens().wait_recv()

    n_groups = digit_a.shape[0]
    position = (
        (seq - back) * rows
        + lax.broadcasted_iota(jnp.int32, (n_groups, TILE), 0) * TILE
        + lax.broadcasted_iota(jnp.int32, (n_groups, TILE), 1)
    )

    ends_step = 8

    def count_ends(k, carry):
        end, ids = carry
        for i in range(ends_step):
            end = end + lens[k * ends_step + i]
            ids = ids + jnp.where(position >= end, 1, 0)
        return end, ids

    _, ids = lax.fori_loop(
        0,
        count * per // ends_step,
        count_ends,
        (jnp.zeros((1, TILE), jnp.int32), jnp.zeros((n_groups, TILE), jnp.int32)),
    )
    digit_a[...] = jnp.where(position < 0, NO_KEY, DIGIT + ids // DIGIT)
    digit_b[...] = jnp.where(position < 0, NO_KEY, ids % DIGIT)

    feature = lax.broadcasted_iota(jnp.int32, (HD, TILE), 0)

    def match(g):
        return (feature == digit_a[g : g + 1, :]) | (feature == digit_b[g : g + 1, :])

    def key_features(g):
        one_hot = jnp.where(match(g), 1.0, 0.0).astype(jnp.bfloat16)
        kf[g * TILE : (g + 1) * TILE, :] = one_hot.T

    for t in range(pieces):
        key_features(own // TILE + t)
        away = jnp.where(match(own // TILE + t), 0.0, -BIG).astype(jnp.bfloat16)
        for i in range(CHUNK // TILE):
            qf[:, t * CHUNK + i * TILE : t * CHUNK + (i + 1) * TILE] = away

    scale = math.log2(math.e) / math.sqrt(HD)
    units = [(a, c, i) for a in range(2) for c in range(kv_heads) for i in range(n_chunks)]
    one = len(units) // 2
    slots = s_buf.shape[0]
    ahead = slots - 1

    def lanes(t, i):
        return pl.ds(pl.multiple_of(t * width, TILE) + i * CHUNK, CHUNK)

    def scores(k, u, t, slabs, first):
        a, c, i = units[u]
        t = t + a
        marks = qf[:, pl.ds(pl.multiple_of(t * CHUNK, TILE), CHUNK)]
        keys = jnp.concatenate(
            [
                jnp.concatenate([kv[pl.ds(at, n), pl.ds(c * HD, HD)], kf[pl.ds(at, n), :]], axis=1)
                for at, n in slabs
            ],
            axis=0,
        )
        queries = jnp.concatenate([qt[c, :, lanes(t, i)], marks], axis=0)
        result = jnp.dot(keys, queries, preferred_element_type=jnp.float32)
        n_keys = result.shape[0]
        if first:
            key = lax.broadcasted_iota(jnp.int32, (TILE, CHUNK), 0)
            query = lax.broadcasted_iota(jnp.int32, (TILE, CHUNK), 1) % TILE
            end = jnp.where(key > query, -BIG, result[n_keys - TILE :])
            result = jnp.concatenate([result[: n_keys - TILE], end], axis=0) if n_keys > TILE else end
        s_buf[k % slots, :n_keys, :] = result
        top = jnp.max(result, axis=0, keepdims=True)
        if not first:
            old_max = m_ref[c, :, lanes(t, i)]
            top = jnp.maximum(old_max, top)
            shrink[k % len(units)] = jnp.exp2((old_max - top) * scale)
        m_now[k % len(units)] = top
        m_ref[c, :, lanes(t, i)] = top

    def weigh(k, u, t, n_keys, first):
        a, c, i = units[u]
        t = t + a
        top = m_now[k % len(units)]
        for r in range(0, n_keys, TILE):
            weights = jnp.exp2((s_buf[k % slots, r : r + TILE, :] - top) * scale)
            p_buf[k % PS, r : r + TILE, :] = weights.astype(jnp.bfloat16)

    def add_values(k, u, t, slabs, first):
        a, c, i = units[u]
        t = t + a
        values = jnp.concatenate(
            [kv[pl.ds(at, n), pl.ds(kv_width + c * HD, HD)].T for at, n in slabs], axis=1
        )
        n_keys = values.shape[1]
        values = jnp.concatenate([values, jnp.ones((16, n_keys), values.dtype)], axis=0)
        weights = p_buf[k % PS, :n_keys, :]
        update = jnp.dot(values, weights, preferred_element_type=jnp.float32)[: HD + 8]
        if first:
            acc[c, :, lanes(t, i)] = update
        else:
            acc[c, :, lanes(t, i)] = acc[c, :, lanes(t, i)] * shrink[k % len(units)] + update

    earlier = list(range(first_key // TILE, own // TILE))
    share = pl.cdiv(len(earlier), pieces - 1)
    events = {2: [(2, 0)], pieces - 2: [(2, 1)], pieces - 1: [(2, 2), (2, 3)]}
    items = [(t, u) for t in range(pieces) for u in range(one)]

    def item(k):
        t, u = items[k]
        return u, t, [(own, (t + 1) * TILE)]

    for k in range(ahead):
        scores(k, *item(k), True)
    for k, (t, u) in enumerate(items):
        if k + ahead < len(items):
            scores(k + ahead, *item(k + ahead), True)
        if k:
            add_values(k - 1, *item(k - 1), True)
        weigh(k, u, t, (t + 1) * TILE, True)
        if u == one - 1:
            for g in earlier[t * share : (t + 1) * share]:
                key_features(g)
            for rel, j in events.get(t, []):
                arrive(rel, j)
    add_values(len(items) - 1, *item(len(items) - 1), True)

    n_step = 4 * TILE
    pairs = pieces // 2
    steps = 5 * pairs - 1

    def where(it):
        it = it + it // (4 * pairs - 1)
        stage = it // pairs
        begin = own - 2 * rows + (stage - stage // 3 * 5) * n_step
        return 2 * (it % pairs), [(pl.multiple_of(begin, TILE), n_step)]

    step_events = {
        0: [(1, 0)],
        1: [(1, 1)],
        2: [(2, 4), (2, 5)],
        3: [(1, 2)],
        4: [(1, 3), (4, 2)],
        5: [(1, 4), (1, 5), (4, 3)],
        6: [(4, 4)],
        7: [(4, 5)],
        8: [(3, 0), (3, 1)],
        10: [(3, 2), (3, 3), (3, 4), (3, 5)],
    }

    def hook(it):
        for low in (0, 4, 8):
            @pl.when(it // 4 == low // 4)
            def _():
                for at, arrivals in step_events.items():
                    if low <= at < low + 4:
                        @pl.when(it == at)
                        def _():
                            for rel, j in arrivals:
                                arrive(rel, j)

    n_units = len(units)
    last = n_units - 1
    for u in range(ahead):
        scores(u, u, *where(0), False)
    p_buf[last % PS] = jnp.zeros(p_buf.shape[1:], p_buf.dtype)
    shrink[last] = jnp.ones((1, CHUNK), jnp.float32)

    def step(it, carry):
        hook(it)
        now, then = where(it), where(it + 1 - (it + 1) // steps)
        before = where(it - (it + steps - 1) // steps)
        for u in range(n_units):
            later = u + ahead
            scores(later, later % n_units, *(now if later < n_units else then), False)
            add_values(u - 1, (u - 1) % n_units, *(now if u else before), False)
            weigh(u, u, now[0], n_step, False)
        return carry

    lax.fori_loop(0, steps, step, 0)
    add_values(last, last, *where(steps - 1), False)

    def finish(t):
        for c in range(kv_heads):
            for g in range(group):
                at = slice(t * width + g * TILE, t * width + (g + 1) * TILE)
                result = (acc[c, :HD, at] * (1.0 / acc[c, HD : HD + 1, at])).astype(jnp.bfloat16)
                columns = slice((c * group + g) * HD, (c * group + g + 1) * HD)
                out_ref[t * TILE : (t + 1) * TILE, columns] = result.T

    ends = [(0, first_key), (4, first_key + n_step)]
    items = [(t, u, [(at, TILE)]) for t, at in ends for u in range(one)]
    others = [t for t in range(pieces) if t not in (0, 4)]
    for k, (t, u, slabs) in enumerate(items[:ahead]):
        scores(k, u, t, slabs, False)
    for k, (t, u, slabs) in enumerate(items):
        if k + ahead < len(items):
            scores(k + ahead, *[items[k + ahead][i] for i in (1, 0, 2)], False)
        weigh(k, u, t, TILE, False)
        add_values(k, u, t, slabs, False)
        if k % 2 and k // 2 < len(others):
            finish(others[k // 2])
    finish(0)
    finish(4)

    for kind, here, there, chunks, to, condition in sends:
        @pl.when(condition)
        def _():
            sent = kv.at[pl.ds(0, len(chunks) * TILE), :]
            pltpu.make_async_remote_copy(
                src_ref=sent,
                dst_ref=sent,
                send_sem=send_sems.at[kind],
                recv_sem=recv_sems.at[0, 0],
                device_id=(to, head),
                device_id_type=MESH,
            ).wait_send()

    all_lens().wait_send()


def body(n_seq, n_head, doc_lengths, queries, key_states, value_states):
    rows, q_width = queries.shape
    pieces = rows // TILE
    kv_heads = key_states.shape[1] // HD
    group = q_width // (kv_heads * HD)
    back = pl.cdiv(LONGEST, rows)
    window = (back + 1) * rows
    per = doc_lengths.shape[0]
    count = n_seq * n_head
    columns = pieces * group * TILE
    units = 2 * kv_heads * group * TILE // CHUNK
    kernel = functools.partial(attend, n_seq, n_head, kv_heads, group)
    return pl.pallas_call(
        kernel,
        out_shape=pltpu.VMEM(queries.shape, jnp.bfloat16),
        in_specs=[pl.BlockSpec(memory_space=pltpu.SMEM)]
        + [pl.BlockSpec(memory_space=pl.ANY)] * 3,
        out_specs=pl.BlockSpec(memory_space=pltpu.VMEM),
        scratch_shapes=[
            pltpu.VMEM((count * per, 1, TILE), jnp.int32),
            pltpu.VMEM((rows, q_width), jnp.bfloat16),
            pltpu.VMEM((window, 2 * kv_heads * HD), jnp.bfloat16),
            pltpu.VMEM((kv_heads, HD, columns), jnp.bfloat16),
            pltpu.VMEM((window, HD), jnp.bfloat16),
            pltpu.VMEM((HD, pieces * CHUNK), jnp.bfloat16),
            pltpu.VMEM((window // TILE, TILE), jnp.int32),
            pltpu.VMEM((window // TILE, TILE), jnp.int32),
            pltpu.VMEM((kv_heads, HD + 8, columns), jnp.float32),
            pltpu.VMEM((kv_heads, 1, columns), jnp.float32),
            pltpu.VMEM((SLOTS, rows, CHUNK), jnp.float32),
            pltpu.VMEM((PS, rows, CHUNK), jnp.bfloat16),
            pltpu.VMEM((units, 1, CHUNK), jnp.float32),
            pltpu.VMEM((units, 1, CHUNK), jnp.float32),
            pltpu.SemaphoreType.DMA((2,)),
            pltpu.SemaphoreType.DMA((2,)),
            pltpu.SemaphoreType.DMA((pieces,)),
            pltpu.SemaphoreType.DMA((9,)),
            pltpu.SemaphoreType.DMA((back + 1, pieces)),
        ],
        compiler_params=pltpu.CompilerParams(
            collective_id=0, has_side_effects=True, vmem_limit_bytes=56 * 1024 * 1024
        ),
    )(doc_lengths, queries, key_states, value_states)


def solution(mesh):
    return jax.shard_map(
        functools.partial(body, mesh.shape["seq"], mesh.shape["head"]),
        mesh=mesh,
        in_specs=(P(("seq", "head")), P("seq", "head"), P("seq", "head"), P("seq", "head")),
        out_specs=P("seq", "head"),
        check_vma=False,
    )
```
